32 devices in a mesh: gx: 4 (over z), gy: 2 (over y), gz: 4 (over x, core).
Axes of the slice: x: 2, y: 2, z: 4, core: 2. Of those that a mesh axis runs over, the one named last changes fastest.
Arguments:
- hidden_acts: bfloat16 [4, 2, 4, 256, 16384], P('gz', 'gy', 'gx'), may hold values from -6 to 6
- output_grad: bfloat16 [4, 2, 4, 256, 32], P('gz', 'gy', 'gx'), may hold values from -6 to 6
- weights: bfloat16 [4, 2, 4, 32, 16384], P('gz', 'gy', 'gx'), may hold values from -6 to 6
- momentum: bfloat16 [4, 2, 4, 32, 16384], P('gz', 'gy', 'gx'), may hold values from -48 to 48
- worker_of_slot: int32 [32], replicated, may hold values from 0 to 31, each once
- round_shift: int32 [8], replicated, may hold values from 0 to 4, as said below
Outputs:
- mixed: bfloat16 [4, 2, 4, 32, 16384], P('gx', 'gy', 'gz')
- new_momentum: bfloat16 [4, 2, 4, 32, 16384], P('gz', 'gy', 'gx')
The draws below stay inside these ranges and needn't reach their ends.
Inputs may be any that keep to these rules, and one draw needn't show every extreme that they name: `round_shift`: each entry is below log2 of 32, so offsets are powers of two below 32; some round has offset 32 / 2 and some round offset 1.
All inputs are finite; a program needn't handle non-finite values.
Results may differ from the reference program's by a relative error of at most 0.0081.
Values may be sent and summed in bfloat16 or wider, within the bound.
A program may use at most 64 MiB of HBM per device.

```python
import jax
import jax.numpy as jnp
from jax import lax

FF = 16384
ROWS = 32
TOK = 256
ROUNDS = 8
WORKERS = 32
N_GX = 4
N_GY = 2
N_GZ = 4


def draw_round_shift(key, part):
    levels = WORKERS.bit_length() - 1
    first_key = jax.random.fold_in(key, 11)
    second_key = jax.random.fold_in(key, 23)
    values = jax.random.randint(first_key, (ROUNDS,), 0, levels, dtype=jnp.int32)
    order = jax.random.permutation(second_key, ROUNDS)
    values = values.at[order[0]].set(jnp.int32(levels - 1))
    values = values.at[order[1]].set(jnp.int32(0))
    return values.astype(jnp.int32)


def shard_levels(rng, shape, split, least, top_value):
    def one(position, shards_of):
        heights = jax.random.uniform(jax.random.fold_in(jax.random.fold_in(rng, 6), position), (shards_of,), jnp.float32, least / len(split), top_value / len(split))
        return jnp.repeat(jnp.exp(heights), shape[position] // shards_of).reshape((-1,) + (1,) * (len(shape) - position - 1))

    level = one(*split[0])
    for cut in split[1:]:
        level = level * one(*cut)
    return level


def scatter_about(key, extent, deviation, most, cuts=(), kind=jnp.bfloat16):
    entries = deviation * jax.random.normal(key, extent, jnp.float32)
    if cuts:
        entries = entries * shard_levels(key, extent, cuts, -0.22, 0.18)
    return jnp.clip(entries, -most, most).astype(kind)


def setup_inputs(seed: int = 0) -> dict:
    seeds = jax.random.split(jax.random.key(seed), 7)
    return {
        "hidden_acts": scatter_about(seeds[0], (N_GZ, N_GY, N_GX, TOK, FF), 1.0, 6.0, ((0, 4), (1, 2), (2, 4))),
        "output_grad": scatter_about(seeds[1], (N_GZ, N_GY, N_GX, TOK, ROWS), 1.0, 6.0, ((0, 4), (1, 2), (2, 4))),
        "weights": scatter_about(seeds[2], (N_GZ, N_GY, N_GX, ROWS, FF), 1.0, 6.0, ((0, 4), (1, 2), (2, 4))),
        "momentum": scatter_about(seeds[3], (N_GZ, N_GY, N_GX, ROWS, FF), 8.0, 48.0, ((0, 4), (1, 2), (2, 4))),
        "worker_of_slot": jax.random.permutation(seeds[4], WORKERS).astype(jnp.int32),
        "round_shift": draw_round_shift(jax.random.fold_in(seeds[6], 71), 0),
    }


learn_rate = 0.01
beta_keep = 0.9


def local_step(items):
    hidden, grad_out, weight, moment = items
    grad = lax.dot_general(grad_out, hidden, (((0,), (0,)), ((), ())), preferred_element_type=jnp.float32)
    velocity = beta_keep * moment.astype(jnp.float32) + grad
    stepped = (weight.astype(jnp.float32) - learn_rate * velocity).astype(jnp.bfloat16)
    return stepped, velocity.astype(jnp.bfloat16)


def reference(hidden_acts, output_grad, weights, momentum, worker_of_slot, round_shift):
    workers = N_GX * N_GY * N_GZ
    hidden = hidden_acts.reshape(workers, TOK, FF)
    grad_out = output_grad.reshape(workers, TOK, ROWS)
    weight = weights.reshape(workers, ROWS, FF)
    moment = momentum.reshape(workers, ROWS, FF)
    stepped, new_moment = lax.map(local_step, (hidden, grad_out, weight, moment))
    replica = jnp.zeros_like(stepped).at[worker_of_slot].set(stepped)
    for step in range(ROUNDS):
        offset = jnp.left_shift(jnp.int32(1), round_shift[step].astype(jnp.int32))
        peer = jnp.roll(replica, offset, axis=0)
        replica = ((replica.astype(jnp.float32) + peer.astype(jnp.float32)) * 0.5).astype(jnp.bfloat16)
    mixed = replica.reshape(N_GX, N_GY, N_GZ, ROWS, FF)
    return mixed, new_moment.reshape(N_GZ, N_GY, N_GX, ROWS, FF)
```

```python
import jax
import jax.numpy as jnp
from jax import lax
from jax.sharding import PartitionSpec as P

learn_rate = 0.01
beta_keep = 0.9
AXES = ("gx", "gy", "gz")


def mixing(held, round_shift, workers):
    rows = jnp.arange(workers, dtype=jnp.int32)
    share = (rows == 0).astype(jnp.float32)
    for step in range(round_shift.shape[0]):
        back = (rows - jnp.left_shift(1, round_shift[step])) % workers
        hit = (back[:, None] == rows[None, :]).astype(jnp.float32)
        share = (share + jnp.sum(hit * share[None, :], axis=1)) * 0.5
    gap = (rows[:, None] - held[None, :]) % workers
    return jnp.sum((gap[:, :, None] == rows) * share, axis=2).astype(jnp.bfloat16)


def shards(hidden_acts, output_grad, weights, momentum, worker_of_slot, round_shift):
    hidden = hidden_acts.reshape(hidden_acts.shape[-2:])
    grad_out = output_grad.reshape(output_grad.shape[-2:])
    weight = weights.reshape(weights.shape[-2:])
    moment = momentum.reshape(momentum.shape[-2:])
    grad = lax.dot_general(
        grad_out, hidden, (((0,), (0,)), ((), ())), preferred_element_type=jnp.float32
    )
    velocity = beta_keep * moment.astype(jnp.float32) + grad
    new_moment = velocity.astype(jnp.bfloat16)
    stepped = (weight.astype(jnp.float32) - learn_rate * velocity).astype(jnp.bfloat16)
    count_x = lax.axis_size("gx")
    count_y = lax.axis_size("gy")
    count_z = lax.axis_size("gz")
    workers = count_x * count_y * count_z
    held = worker_of_slot.reshape(count_z, count_y, count_x).transpose(2, 1, 0).reshape(-1)
    matrix = mixing(held, round_shift, workers)
    pieces = stepped.reshape(workers, stepped.size // workers)
    got = lax.all_to_all(pieces, AXES, split_axis=0, concat_axis=0, tiled=True)
    mixed = lax.dot_general(
        matrix, got, (((1,), (0,)), ((), ())), preferred_element_type=jnp.float32
    ).astype(jnp.bfloat16)
    block = lax.all_to_all(mixed, AXES, split_axis=0, concat_axis=0, tiled=True)
    return (block.reshape(weights.shape), new_moment.reshape(momentum.shape))


def solution(mesh):
    placed = (
        P("gz", "gy", "gx", None, None),
        P("gz", "gy", "gx", None, None),
        P("gz", "gy", "gx", None, None),
        P("gz", "gy", "gx", None, None),
        P(),
        P(),
    )
    return jax.shard_map(
        shards,
        mesh=mesh,
        in_specs=placed,
        out_specs=(P("gx", "gy", "gz", None, None), P("gz", "gy", "gx", None, None)),
        check_vma=False,
    )
```

```python
import functools

import jax
import jax.numpy as jnp
from jax import lax
from jax.experimental import pallas as pl
from jax.experimental.pallas import tpu as pltpu
from jax.sharding import PartitionSpec as P

learn_rate = 0.01
beta_keep = 0.9
TILE = 16
MESH = pl.DeviceIdType.MESH


def iota(shape, axis):
    return lax.broadcasted_iota(jnp.int32, shape, axis)


def ones_where(mask):
    return jnp.where(mask, 1.0, 0.0).astype(jnp.bfloat16)


def exact_dot(a, b):
    return jnp.dot(a, b, preferred_element_type=jnp.float32)


def kernel(
    sizes,
    hidden_hbm,
    grad_ref,
    weight_hbm,
    moment_hbm,
    held_ref,
    shift_ref,
    out_ref,
    new_moment_ref,
    hidden,
    weight,
    moment,
    stage,
    recv,
    mixed,
    spread,
    hidden_sem,
    local_sem,
    send_sem,
    recv_sem,
    back_send_sem,
    back_recv_sem,
):
    size_x, size_y, size_z = sizes
    workers = size_x * size_y * size_z
    columns, _, width = hidden.shape
    parts = out_ref.shape[0] // TILE
    chunks = recv.shape[0]
    rounds = shift_ref.shape[0]
    my_x, my_y, my_z = lax.axis_index("gx"), lax.axis_index("gy"), lax.axis_index("gz")
    me = (my_x * size_y + my_y) * size_z + my_z
    slot = my_x + size_x * (my_y + size_y * my_z)
    half_x = size_x // 2

    def target(step):
        per = workers // 2
        far = 1 - lax.div(step, per)
        rest = lax.rem(step, per)
        side = lax.div(my_x, half_x)
        other = far + side - 2 * far * side
        to_x = other * half_x + lax.rem(my_x + lax.div(rest, size_y * size_z), half_x)
        to_y = lax.rem(my_y + lax.rem(lax.div(rest, size_z), size_y), size_y)
        to_z = lax.rem(my_z + lax.rem(rest, size_z), size_z)
        return (to_x * size_y + to_y) * size_z + to_z

    def coordinates(device):
        return {
            "gx": lax.div(device, size_y * size_z),
            "gy": lax.rem(lax.div(device, size_z), size_y),
            "gz": lax.rem(device, size_z),
        }

    def column(step):
        return target(step) if columns == workers else lax.rem(me + step, columns)

    def load(step):
        place = column(step)
        return pltpu.make_async_copy(
            hidden_hbm.at[:, pl.ds(pl.multiple_of(place * width, 128), width)],
            hidden.at[place],
            hidden_sem.at[step],
        )

    weight_copy = pltpu.make_async_copy(weight_hbm, weight, local_sem.at[0])
    moment_copy = pltpu.make_async_copy(moment_hbm, moment, local_sem.at[1])
    weight_copy.start()
    moment_copy.start()
    lax.fori_loop(0, columns, lambda step, c: (load(step).start(), c)[1], 0)

    barrier = pltpu.get_barrier_semaphore()

    def greet(step, carry):
        device = target(step)

        @pl.when(device != me)
        def _():
            pl.semaphore_signal(
                barrier, inc=1, device_id=coordinates(device), device_id_type=MESH
            )

        return carry

    lax.fori_loop(0, workers, greet, 0)
    grad_rows = jnp.transpose(grad_ref[...].astype(jnp.float32)).astype(jnp.bfloat16)
    weight_copy.wait()
    moment_copy.wait()
    pl.semaphore_wait(barrier, workers - 1)

    def place_of(part, where):
        block = part * columns
        return block // workers, block % workers + where

    def send(part, where):
        chunk, device = place_of(part, where)

        @pl.when(device != me)
        def _():
            pltpu.make_async_remote_copy(
                src_ref=stage.at[part, where],
                dst_ref=recv.at[chunk, slot],
                send_sem=send_sem.at[chunk],
                recv_sem=recv_sem.at[chunk],
                device_id=coordinates(device),
                device_id_type=MESH,
            ).start()

    early = [part for part in range(parts) if place_of(part, 0)[0] == 0]
    late = [part for part in range(parts) if place_of(part, 0)[0] > 0]

    def compute(step, carry):
        where = column(step)
        load(step).wait()
        span = pl.ds(pl.multiple_of(where * width, 128), width)
        grad = exact_dot(grad_rows, hidden[where])
        velocity = beta_keep * moment[:, span].astype(jnp.float32) + grad
        new_moment_ref[:, span] = velocity.astype(jnp.bfloat16)
        stepped = (weight[:, span].astype(jnp.float32) - learn_rate * velocity).astype(
            jnp.bfloat16
        )
        for part in range(parts):
            piece = stepped[part * TILE : (part + 1) * TILE]
            stage[part, where] = piece
            chunk, device = place_of(part, where)

            @pl.when(device == me)
            def _():
                recv[chunk, slot] = piece

        @pl.when(step > 0)
        def _():
            for part in early:
                send(part, column(step - 1))

        return carry

    lax.fori_loop(0, columns, compute, 0)
    for part in early:
        send(part, column(jnp.int32(columns - 1)))
    for part in late:
        lax.fori_loop(0, columns, lambda step, c: (send(part, column(step)), c)[1], 0)

    square = (workers, workers)
    gap = lax.rem(iota(square, 0) - iota(square, 1) + workers, workers)
    level = jnp.full(square, -1, jnp.int32)
    for power in range(workers.bit_length() - 1):
        level = jnp.where(gap == 1 << power, power, level)
    table = ones_where(held_ref[...] == iota(square, 0))
    for step in range(rounds):
        turn = ones_where((gap == 0) | (level == shift_ref[step]))
        table = exact_dot(turn, table).astype(jnp.bfloat16)
    distinct = workers // 2
    table = (table[:distinct].astype(jnp.float32) * 0.5**rounds).astype(jnp.bfloat16)
    wide = (workers, workers * TILE)
    table = exact_dot(table, ones_where(iota(wide, 1) // TILE == iota(wide, 0))).astype(
        jnp.bfloat16
    )
    height = min(256, distinct * TILE)

    def fill(step, carry):
        tall = (height, distinct)
        pick = ones_where((iota(tall, 0) + step * height) // TILE == iota(tall, 1))
        full = (height, workers * TILE)
        same = iota(full, 0) % TILE == iota(full, 1) % TILE
        spread[pl.ds(pl.multiple_of(step * height, height), height), :] = jnp.where(
            same, exact_dot(pick, table), 0.0
        ).astype(jnp.bfloat16)
        return carry

    lax.fori_loop(0, distinct * TILE // height, fill, 0)

    def pieces_wait(sem):
        ref = recv.at[0, pl.ds(0, workers - 1)]
        pltpu.make_async_copy(ref, ref, sem).wait()

    for chunk in range(chunks):
        pieces_wait(recv_sem.at[chunk])
        got = recv[chunk].reshape(workers * TILE, width)

        def blend(step, carry):
            result = exact_dot(
                spread[pl.ds(pl.multiple_of(step * height, height), height), :], got
            )
            mixed[chunk, pl.ds(step * (height // TILE), height // TILE)] = result.astype(
                jnp.bfloat16
            ).reshape(height // TILE, TILE, width)
            return carry

        lax.fori_loop(0, distinct * TILE // height, blend, 0)
        block = chunk * workers + me
        row = pl.multiple_of(lax.div(block, columns) * TILE, TILE)
        first = pl.multiple_of(lax.rem(block, columns) * width, 128)
        mine = (pl.ds(row, TILE), pl.ds(first, width))
        out_ref[mine] = mixed[chunk, lax.rem(me, distinct)]

        def back(step, carry):
            device = target(step)

            @pl.when(device != me)
            def _():
                pltpu.make_async_remote_copy(
                    src_ref=mixed.at[chunk, lax.rem(device, distinct)],
                    dst_ref=out_ref.at[mine],
                    send_sem=back_send_sem.at[chunk],
                    recv_sem=back_recv_sem.at[chunk],
                    device_id=coordinates(device),
                    device_id_type=MESH,
                ).start()

            return carry

        lax.fori_loop(0, workers, back, 0)

    for chunk in range(chunks):
        pieces_wait(send_sem.at[chunk])
        pieces_wait(back_send_sem.at[chunk])
        pieces_wait(back_recv_sem.at[chunk])


def shards(sizes, hidden_acts, output_grad, weights, momentum, worker_of_slot, round_shift):
    hidden = hidden_acts.reshape(hidden_acts.shape[-2:])
    grad_out = output_grad.reshape(output_grad.shape[-2:])
    weight = weights.reshape(weights.shape[-2:])
    moment = momentum.reshape(momentum.shape[-2:])
    workers = sizes[0] * sizes[1] * sizes[2]
    tokens, features = hidden.shape
    rows = weight.shape[0]
    parts = rows // TILE
    width = max(128, features // workers)
    columns = features // width
    chunks = parts * columns // workers
    distinct = workers // 2
    anywhere = pl.BlockSpec(memory_space=pl.ANY)
    vmem = pl.BlockSpec(memory_space=pltpu.VMEM)
    smem = pl.BlockSpec(memory_space=pltpu.SMEM)
    half = jnp.bfloat16
    mixed, new_moment = pl.pallas_call(
        functools.partial(kernel, sizes),
        out_shape=[jax.ShapeDtypeStruct((rows, features), half)] * 2,
        in_specs=[anywhere, vmem, anywhere, anywhere, vmem, smem],
        out_specs=[vmem, vmem],
        scratch_shapes=[
            pltpu.VMEM((columns, tokens, width), half),
            pltpu.VMEM((rows, features), half),
            pltpu.VMEM((rows, features), half),
            pltpu.VMEM((parts, columns, TILE, width), half),
            pltpu.VMEM((chunks, workers, TILE, width), half),
            pltpu.VMEM((chunks, distinct, TILE, width), half),
            pltpu.VMEM((distinct * TILE, workers * TILE), half),
            pltpu.SemaphoreType.DMA((columns,)),
            pltpu.SemaphoreType.DMA((2,)),
            pltpu.SemaphoreType.DMA((chunks,)),
            pltpu.SemaphoreType.DMA((chunks,)),
            pltpu.SemaphoreType.DMA((chunks,)),
            pltpu.SemaphoreType.DMA((chunks,)),
        ],
        compiler_params=pltpu.CompilerParams(
            collective_id=0, has_side_effects=True, vmem_limit_bytes=60 * 1024 * 1024
        ),
        name="step_and_gossip",
    )(hidden, grad_out, weight, moment, worker_of_slot.reshape(1, workers), round_shift)
    return (mixed.reshape(weights.shape), new_moment.reshape(momentum.shape))


def solution(mesh):
    sizes = (mesh.shape["gx"], mesh.shape["gy"], mesh.shape["gz"])
    placed = (
        P("gz", "gy", "gx", None, None),
        P("gz", "gy", "gx", None, None),
        P("gz", "gy", "gx", None, None),
        P("gz", "gy", "gx", None, None),
        P(),
        P(),
    )
    return jax.shard_map(
        functools.partial(shards, sizes),
        mesh=mesh,
        in_specs=placed,
        out_specs=(P("gx", "gy", "gz", None, None), P("gz", "gy", "gx", None, None)),
        check_vma=False,
    )
```

```python
import functools

import jax
import jax.numpy as jnp
from jax import lax
from jax.experimental import pallas as pl
from jax.experimental.pallas import tpu as pltpu
from jax.sharding import PartitionSpec as P

learn_rate = 0.01
beta_keep = 0.9
TILE = 16
GROUP = 2
MESH = pl.DeviceIdType.MESH


def iota(shape, axis):
    return lax.broadcasted_iota(jnp.int32, shape, axis)


def ones_where(mask):
    return jnp.where(mask, 1.0, 0.0).astype(jnp.bfloat16)


def exact_dot(a, b):
    return jnp.dot(a, b, preferred_element_type=jnp.float32)


def kernel(
    sizes,
    hidden_hbm,
    grad_ref,
    weight_hbm,
    moment_hbm,
    held_ref,
    shift_ref,
    out_ref,
    new_moment_ref,
    hidden,
    weight,
    moment,
    stage,
    recv,
    mixed,
    spread,
    hidden_sem,
    moment_sem,
    weight_sem,
    send_sem,
    recv_sem,
    back_send_sem,
    back_recv_sem,
):
    size_x, size_y, size_z = sizes
    workers = size_x * size_y * size_z
    columns, _, width = hidden.shape
    parts = out_ref.shape[0] // TILE
    chunks = recv.shape[0]
    rounds = shift_ref.shape[0]
    my_x, my_y, my_z = lax.axis_index("gx"), lax.axis_index("gy"), lax.axis_index("gz")
    me = (my_x * size_y + my_y) * size_z + my_z
    slot = my_x + size_x * (my_y + size_y * my_z)
    half_x = size_x // 2

    def target(step):
        per = workers // 2
        far = 1 - lax.div(step, per)
        rest = lax.rem(step, per)
        side = lax.div(my_x, half_x)
        other = far + side - 2 * far * side
        to_x = other * half_x + lax.rem(my_x + lax.div(rest, size_y * size_z), half_x)
        to_y = lax.rem(my_y + lax.rem(lax.div(rest, size_z), size_y), size_y)
        to_z = lax.rem(my_z + lax.rem(rest, size_z), size_z)
        return (to_x * size_y + to_y) * size_z + to_z

    def coordinates(device):
        return {
            "gx": lax.div(device, size_y * size_z),
            "gy": lax.rem(lax.div(device, size_z), size_y),
            "gz": lax.rem(device, size_z),
        }

    def column(step):
        return target(step) if columns == workers else lax.rem(me + step, columns)

    def loads(step):
        place = column(step)
        span = pl.ds(pl.multiple_of(place * width, 128), width)
        return [
            pltpu.make_async_copy(source.at[:, span], kept.at[place], sem.at[step])
            for source, kept, sem in (
                (hidden_hbm, hidden, hidden_sem),
                (moment_hbm, moment, moment_sem),
                (weight_hbm, weight, weight_sem),
            )
        ]

    def load(step, carry):
        for copy in loads(step):
            copy.start()
        return carry

    barrier = pltpu.get_barrier_semaphore()

    def greet(step, carry):
        device = target(step)

        @pl.when(device != me)
        def _():
            pl.semaphore_signal(
                barrier, inc=1, device_id=coordinates(device), device_id_type=MESH
            )

        return carry

    lax.fori_loop(0, workers, greet, 0)
    lax.fori_loop(0, columns, load, 0)
    grad_rows = grad_ref[...]
    def place_of(part, where):
        block = part * columns
        return block // workers, block % workers + where

    def send(part, where):
        chunk, device = place_of(part, where)

        @pl.when(device != me)
        def _():
            pltpu.make_async_remote_copy(
                src_ref=stage.at[part, where],
                dst_ref=recv.at[chunk, slot],
                send_sem=send_sem.at[chunk],
                recv_sem=recv_sem.at[chunk],
                device_id=coordinates(device),
                device_id_type=MESH,
            ).start()

    early = [part for part in range(parts) if place_of(part, 0)[0] == 0]
    late = [part for part in range(parts) if place_of(part, 0)[0] > 0]

    def compute(group):
        steps = [group * GROUP + k for k in range(GROUP)]
        for step in steps:
            for copy in loads(step):
                copy.wait()
        places = [column(step) for step in steps]
        grads = [exact_dot(grad_rows, hidden[where]) for where in places]
        for where, grad in zip(places, grads):
            span = pl.ds(pl.multiple_of(where * width, 128), width)
            velocity = beta_keep * moment[where].astype(jnp.float32) + grad
            new_moment_ref[:, span] = velocity.astype(jnp.bfloat16)
            stepped = (weight[where].astype(jnp.float32) - learn_rate * velocity).astype(
                jnp.bfloat16
            )
            for part in range(parts):
                piece = stepped[part * TILE : (part + 1) * TILE]
                stage[part, where] = piece
                chunk, device = place_of(part, where)

                @pl.when(device == me)
                def _():
                    recv[chunk, slot] = piece

    def send_early(group):
        for k in range(GROUP):
            for part in early:
                send(part, column(group * GROUP + k))

    def compute_and_send(group, carry):
        compute(group)
        send_early(group - 1)
        return carry

    groups = columns // GROUP
    compute(jnp.int32(0))
    pl.semaphore_wait(barrier, workers - 1)
    send_early(jnp.int32(0))
    compute(jnp.int32(1))
    lax.fori_loop(2, groups, compute_and_send, 0)
    send_early(jnp.int32(groups - 1))
    for part in late:
        lax.fori_loop(0, columns, lambda step, c: (send(part, column(step)), c)[1], 0)

    square = (workers, workers)
    gap = lax.rem(iota(square, 0) - iota(square, 1) + workers, workers)
    level = jnp.full(square, -1, jnp.int32)
    for power in range(workers.bit_length() - 1):
        level = jnp.where(gap == 1 << power, power, level)
    table = ones_where(held_ref[...] == iota(square, 0))
    for step in range(rounds):
        turn = ones_where((gap == 0) | (level == shift_ref[step]))
        table = exact_dot(turn, table).astype(jnp.bfloat16)
    distinct = workers // 2
    table = (table[:distinct].astype(jnp.float32) * 0.5**rounds).astype(jnp.bfloat16)
    wide = (workers, workers * TILE)
    table = exact_dot(table, ones_where(iota(wide, 1) // TILE == iota(wide, 0))).astype(
        jnp.bfloat16
    )
    height = min(256, distinct * TILE)

    def fill(step, carry):
        tall = (height, distinct)
        pick = ones_where((iota(tall, 0) + step * height) // TILE == iota(tall, 1))
        full = (height, workers * TILE)
        same = iota(full, 0) % TILE == iota(full, 1) % TILE
        spread[pl.ds(pl.multiple_of(step * height, height), height), :] = jnp.where(
            same, exact_dot(pick, table), 0.0
        ).astype(jnp.bfloat16)
        return carry

    lax.fori_loop(0, distinct * TILE // height, fill, 0)

    def pieces_wait(sem):
        ref = recv.at[0, pl.ds(0, workers - 1)]
        pltpu.make_async_copy(ref, ref, sem).wait()

    for chunk in range(chunks):
        pieces_wait(recv_sem.at[chunk])
        got = recv[chunk].reshape(workers * TILE, width)

        def blend(step, carry):
            result = exact_dot(
                spread[pl.ds(pl.multiple_of(step * height, height), height), :], got
            )
            mixed[chunk, pl.ds(step * (height // TILE), height // TILE)] = result.astype(
                jnp.bfloat16
            ).reshape(height // TILE, TILE, width)
            return carry

        lax.fori_loop(0, distinct * TILE // height, blend, 0)
        block = chunk * workers + me
        row = pl.multiple_of(lax.div(block, columns) * TILE, TILE)
        first = pl.multiple_of(lax.rem(block, columns) * width, 128)
        mine = (pl.ds(row, TILE), pl.ds(first, width))
        out_ref[mine] = mixed[chunk, lax.rem(me, distinct)]

        def back(step, carry):
            device = target(step)

            @pl.when(device != me)
            def _():
                pltpu.make_async_remote_copy(
                    src_ref=mixed.at[chunk, lax.rem(device, distinct)],
                    dst_ref=out_ref.at[mine],
                    send_sem=back_send_sem.at[chunk],
                    recv_sem=back_recv_sem.at[chunk],
                    device_id=coordinates(device),
                    device_id_type=MESH,
                ).start()

            return carry

        lax.fori_loop(0, workers, back, 0)

    for chunk in range(chunks):
        pieces_wait(send_sem.at[chunk])
        pieces_wait(back_send_sem.at[chunk])
        pieces_wait(back_recv_sem.at[chunk])


def store(mixed_ref, moment_ref, mixed_hbm, moment_hbm, sem):
    copies = [
        pltpu.make_async_copy(mixed_ref, mixed_hbm, sem.at[0]),
        pltpu.make_async_copy(moment_ref, moment_hbm, sem.at[1]),
    ]
    for copy in copies:
        copy.start()
    for copy in copies:
        copy.wait()


def shards(sizes, hidden_acts, output_grad, weights, momentum, worker_of_slot, round_shift):
    hidden = hidden_acts.reshape(hidden_acts.shape[-2:])
    grad_out = output_grad.reshape(output_grad.shape[-2:]).T
    weight = weights.reshape(weights.shape[-2:])
    moment = momentum.reshape(momentum.shape[-2:])
    workers = sizes[0] * sizes[1] * sizes[2]
    tokens, features = hidden.shape
    rows = weight.shape[0]
    parts = rows // TILE
    width = max(128, features // workers)
    columns = features // width
    chunks = parts * columns // workers
    distinct = workers // 2
    anywhere = pl.BlockSpec(memory_space=pl.ANY)
    vmem = pl.BlockSpec(memory_space=pltpu.VMEM)
    smem = pl.BlockSpec(memory_space=pltpu.SMEM)
    half = jnp.bfloat16
    mixed, new_moment = pl.pallas_call(
        functools.partial(kernel, sizes),
        out_shape=[pltpu.VMEM((rows, features), half)] * 2,
        in_specs=[anywhere, vmem, anywhere, anywhere, vmem, smem],
        out_specs=[vmem, vmem],
        scratch_shapes=[
            pltpu.VMEM((columns, tokens, width), half),
            pltpu.VMEM((columns, rows, width), half),
            pltpu.VMEM((columns, rows, width), half),
            pltpu.VMEM((parts, columns, TILE, width), half),
            pltpu.VMEM((chunks, workers, TILE, width), half),
            pltpu.VMEM((chunks, distinct, TILE, width), half),
            pltpu.VMEM((distinct * TILE, workers * TILE), half),
            pltpu.SemaphoreType.DMA((columns,)),
            pltpu.SemaphoreType.DMA((columns,)),
            pltpu.SemaphoreType.DMA((columns,)),
            pltpu.SemaphoreType.DMA((chunks,)),
            pltpu.SemaphoreType.DMA((chunks,)),
            pltpu.SemaphoreType.DMA((chunks,)),
            pltpu.SemaphoreType.DMA((chunks,)),
        ],
        compiler_params=pltpu.CompilerParams(
            collective_id=0, has_side_effects=True, vmem_limit_bytes=60 * 1024 * 1024
        ),
        name="step_and_gossip",
    )(hidden, grad_out, weight, moment, worker_of_slot.reshape(1, workers), round_shift)
    mixed, new_moment = pl.pallas_call(
        store,
        out_shape=[jax.ShapeDtypeStruct((rows, features), half)] * 2,
        in_specs=[anywhere, anywhere],
        out_specs=[anywhere, anywhere],
        scratch_shapes=[pltpu.SemaphoreType.DMA((2,))],
        name="store",
    )(
        pltpu.with_memory_space_constraint(mixed, pltpu.VMEM),
        pltpu.with_memory_space_constraint(new_moment, pltpu.VMEM),
    )
    return (mixed.reshape(weights.shape), new_moment.reshape(momentum.shape))


def solution(mesh):
    sizes = (mesh.shape["gx"], mesh.shape["gy"], mesh.shape["gz"])
    placed = (
        P("gz", "gy", "gx", None, None),
        P("gz", "gy", "gx", None, None),
        P("gz", "gy", "gx", None, None),
        P("gz", "gy", "gx", None, None),
        P(),
        P(),
    )
    return jax.shard_map(
        functools.partial(shards, sizes),
        mesh=mesh,
        in_specs=placed,
        out_specs=(P("gx", "gy", "gz", None, None), P("gz", "gy", "gx", None, None)),
        check_vma=False,
    )
```

```python
import functools

import jax
import jax.numpy as jnp
from jax import lax
from jax.experimental import pallas as pl
from jax.experimental.pallas import tpu as pltpu
from jax.sharding import PartitionSpec as P

learn_rate = 0.01
beta_keep = 0.9
TILE = 16
GROUP = 2
MESH = pl.DeviceIdType.MESH


def iota(shape, axis):
    return lax.broadcasted_iota(jnp.int32, shape, axis)


def ones_where(mask):
    return jnp.where(mask, 1.0, 0.0).astype(jnp.bfloat16)


def exact_dot(a, b):
    return jnp.dot(a, b, preferred_element_type=jnp.float32)


def kernel(
    sizes,
    hidden_hbm,
    grad_ref,
    weight_hbm,
    moment_hbm,
    held_ref,
    shift_ref,
    out_ref,
    new_moment_ref,
    hidden,
    weight,
    moment,
    stage,
    recv,
    mixed,
    spread,
    hidden_sem,
    moment_sem,
    weight_sem,
    send_sem,
    recv_sem,
    back_send_sem,
    back_recv_sem,
):
    size_x, size_y, size_z = sizes
    workers = size_x * size_y * size_z
    columns, _, width = hidden.shape
    parts = out_ref.shape[0] // TILE
    chunks = recv.shape[0]
    rounds = shift_ref.shape[0]
    my_x, my_y, my_z = lax.axis_index("gx"), lax.axis_index("gy"), lax.axis_index("gz")
    me = (my_x * size_y + my_y) * size_z + my_z
    slot = my_x + size_x * (my_y + size_y * my_z)
    half_x = size_x // 2

    def target(step):
        per = workers // 2
        far = 1 - lax.div(step, per)
        rest = lax.rem(step, per)
        side = lax.div(my_x, half_x)
        other = far + side - 2 * far * side
        to_y = lax.rem(my_y + lax.rem(rest, size_y), size_y)
        to_z = lax.rem(my_z + lax.rem(lax.div(rest, size_y), size_z), size_z)
        to_x = other * half_x + lax.rem(my_x + lax.div(rest, size_y * size_z), half_x)
        return (to_x * size_y + to_y) * size_z + to_z

    def coordinates(device):
        return {
            "gx": lax.div(device, size_y * size_z),
            "gy": lax.rem(lax.div(device, size_z), size_y),
            "gz": lax.rem(device, size_z),
        }

    def column(step):
        return target(step) if columns == workers else lax.rem(me + step, columns)

    def loads(step):
        place = column(step)
        span = pl.ds(pl.multiple_of(place * width, 128), width)
        return [
            pltpu.make_async_copy(source.at[:, span], kept.at[place], sem.at[step])
            for source, kept, sem in (
                (hidden_hbm, hidden, hidden_sem),
                (moment_hbm, moment, moment_sem),
                (weight_hbm, weight, weight_sem),
            )
        ]

    def load(step, carry):
        for copy in loads(step):
            copy.start()
        return carry

    barrier = pltpu.get_barrier_semaphore()

    def greet(step, carry):
        device = target(step)

        @pl.when(device != me)
        def _():
            pl.semaphore_signal(
                barrier, inc=1, device_id=coordinates(device), device_id_type=MESH
            )

        return carry

    lax.fori_loop(0, workers, greet, 0)
    lax.fori_loop(0, columns, load, 0)
    grad_rows = grad_ref[...]
    def place_of(part, where):
        block = part * columns
        return block // workers, block % workers + where

    def send(part, where):
        chunk, device = place_of(part, where)

        @pl.when(device != me)
        def _():
            pltpu.make_async_remote_copy(
                src_ref=stage.at[part, where],
                dst_ref=recv.at[chunk, slot],
                send_sem=send_sem.at[chunk],
                recv_sem=recv_sem.at[chunk],
                device_id=coordinates(device),
                device_id_type=MESH,
            ).start()

    early = [part for part in range(parts) if place_of(part, 0)[0] == 0]
    late = [part for part in range(parts) if place_of(part, 0)[0] > 0]

    def compute(group):
        steps = [group * GROUP + k for k in range(GROUP)]
        for step in steps:
            for copy in loads(step):
                copy.wait()
        places = [column(step) for step in steps]
        grads = [exact_dot(grad_rows, hidden[where]) for where in places]
        for where, grad in zip(places, grads):
            span = pl.ds(pl.multiple_of(where * width, 128), width)
            velocity = beta_keep * moment[where].astype(jnp.float32) + grad
            new_moment_ref[:, span] = velocity.astype(jnp.bfloat16)
            stepped = (weight[where].astype(jnp.float32) - learn_rate * velocity).astype(
                jnp.bfloat16
            )
            for part in range(parts):
                piece = stepped[part * TILE : (part + 1) * TILE]
                stage[part, where] = piece
                chunk, device = place_of(part, where)

                @pl.when(device == me)
                def _():
                    recv[chunk, slot] = piece

    def send_early(group):
        for k in range(GROUP):
            for part in early:
                send(part, column(group * GROUP + k))

    def compute_and_send(group, carry):
        compute(group)
        send_early(group - 1)
        return carry

    groups = columns // GROUP
    compute(jnp.int32(0))
    pl.semaphore_wait(barrier, workers - 1)
    send_early(jnp.int32(0))
    compute(jnp.int32(1))
    lax.fori_loop(2, groups, compute_and_send, 0)
    send_early(jnp.int32(groups - 1))
    for part in late:
        lax.fori_loop(0, columns, lambda step, c: (send(part, column(step)), c)[1], 0)

    square = (workers, workers)
    gap = lax.rem(iota(square, 0) - iota(square, 1) + workers, workers)
    level = jnp.full(square, -1, jnp.int32)
    for power in range(workers.bit_length() - 1):
        level = jnp.where(gap == 1 << power, power, level)
    table = ones_where(held_ref[...] == iota(square, 0))
    for step in range(rounds):
        turn = ones_where((gap == 0) | (level == shift_ref[step]))
        table = exact_dot(turn, table).astype(jnp.bfloat16)
    distinct = workers // 2
    table = (table[:distinct].astype(jnp.float32) * 0.5**rounds).astype(jnp.bfloat16)
    wide = (workers, workers * TILE)
    table = exact_dot(table, ones_where(iota(wide, 1) // TILE == iota(wide, 0))).astype(
        jnp.bfloat16
    )
    height = min(256, distinct * TILE)

    def fill(step, carry):
        tall = (height, distinct)
        pick = ones_where((iota(tall, 0) + step * height) // TILE == iota(tall, 1))
        full = (height, workers * TILE)
        same = iota(full, 0) % TILE == iota(full, 1) % TILE
        spread[pl.ds(pl.multiple_of(step * height, height), height), :] = jnp.where(
            same, exact_dot(pick, table), 0.0
        ).astype(jnp.bfloat16)
        return carry

    lax.fori_loop(0, distinct * TILE // height, fill, 0)

    def pieces_wait(sem):
        ref = recv.at[0, pl.ds(0, workers - 1)]
        pltpu.make_async_copy(ref, ref, sem).wait()

    for chunk in range(chunks):
        pieces_wait(recv_sem.at[chunk])
        got = recv[chunk].reshape(workers * TILE, width)

        def blend(step, carry):
            result = exact_dot(
                spread[pl.ds(pl.multiple_of(step * height, height), height), :], got
            )
            mixed[chunk, pl.ds(step * (height // TILE), height // TILE)] = result.astype(
                jnp.bfloat16
            ).reshape(height // TILE, TILE, width)
            return carry

        lax.fori_loop(0, distinct * TILE // height, blend, 0)
        block = chunk * workers + me
        row = pl.multiple_of(lax.div(block, columns) * TILE, TILE)
        first = pl.multiple_of(lax.rem(block, columns) * width, 128)
        mine = (pl.ds(row, TILE), pl.ds(first, width))
        out_ref[mine] = mixed[chunk, lax.rem(me, distinct)]

        turned = workers // 2 if chunk == chunks - 1 else 0

        def back(step, carry):
            device = target(lax.rem(step + turned, workers))

            @pl.when(device != me)
            def _():
                pltpu.make_async_remote_copy(
                    src_ref=mixed.at[chunk, lax.rem(device, distinct)],
                    dst_ref=out_ref.at[mine],
                    send_sem=back_send_sem.at[chunk],
                    recv_sem=back_recv_sem.at[chunk],
                    device_id=coordinates(device),
                    device_id_type=MESH,
                ).start()

            return carry

        lax.fori_loop(0, workers, back, 0)

    for chunk in range(chunks):
        pieces_wait(send_sem.at[chunk])
        pieces_wait(back_send_sem.at[chunk])
        pieces_wait(back_recv_sem.at[chunk])


def store(mixed_ref, moment_ref, mixed_hbm, moment_hbm, sem):
    copies = [
        pltpu.make_async_copy(mixed_ref, mixed_hbm, sem.at[0]),
        pltpu.make_async_copy(moment_ref, moment_hbm, sem.at[1]),
    ]
    for copy in copies:
        copy.start()
    for copy in copies:
        copy.wait()


def shards(sizes, hidden_acts, output_grad, weights, momentum, worker_of_slot, round_shift):
    hidden = hidden_acts.reshape(hidden_acts.shape[-2:])
    grad_out = output_grad.reshape(output_grad.shape[-2:]).T
    weight = weights.reshape(weights.shape[-2:])
    moment = momentum.reshape(momentum.shape[-2:])
    workers = sizes[0] * sizes[1] * sizes[2]
    tokens, features = hidden.shape
    rows = weight.shape[0]
    parts = rows // TILE
    width = max(128, features // workers)
    columns = features // width
    chunks = parts * columns // workers
    distinct = workers // 2
    anywhere = pl.BlockSpec(memory_space=pl.ANY)
    vmem = pl.BlockSpec(memory_space=pltpu.VMEM)
    smem = pl.BlockSpec(memory_space=pltpu.SMEM)
    half = jnp.bfloat16
    mixed, new_moment = pl.pallas_call(
        functools.partial(kernel, sizes),
        out_shape=[pltpu.VMEM((rows, features), half)] * 2,
        in_specs=[anywhere, vmem, anywhere, anywhere, vmem, smem],
        out_specs=[vmem, vmem],
        scratch_shapes=[
            pltpu.VMEM((columns, tokens, width), half),
            pltpu.VMEM((columns, rows, width), half),
            pltpu.VMEM((columns, rows, width), half),
            pltpu.VMEM((parts, columns, TILE, width), half),
            pltpu.VMEM((chunks, workers, TILE, width), half),
            pltpu.VMEM((chunks, distinct, TILE, width), half),
            pltpu.VMEM((distinct * TILE, workers * TILE), half),
            pltpu.SemaphoreType.DMA((columns,)),
            pltpu.SemaphoreType.DMA((columns,)),
            pltpu.SemaphoreType.DMA((columns,)),
            pltpu.SemaphoreType.DMA((chunks,)),
            pltpu.SemaphoreType.DMA((chunks,)),
            pltpu.SemaphoreType.DMA((chunks,)),
            pltpu.SemaphoreType.DMA((chunks,)),
        ],
        compiler_params=pltpu.CompilerParams(
            collective_id=0, has_side_effects=True, vmem_limit_bytes=60 * 1024 * 1024
        ),
        name="step_and_gossip",
    )(hidden, grad_out, weight, moment, worker_of_slot.reshape(1, workers), round_shift)
    mixed, new_moment = pl.pallas_call(
        store,
        out_shape=[jax.ShapeDtypeStruct((rows, features), half)] * 2,
        in_specs=[anywhere, anywhere],
        out_specs=[anywhere, anywhere],
        scratch_shapes=[pltpu.SemaphoreType.DMA((2,))],
        name="store",
    )(
        pltpu.with_memory_space_constraint(mixed, pltpu.VMEM),
        pltpu.with_memory_space_constraint(new_moment, pltpu.VMEM),
    )
    return (mixed.reshape(weights.shape), new_moment.reshape(momentum.shape))


def solution(mesh):
    sizes = (mesh.shape["gx"], mesh.shape["gy"], mesh.shape["gz"])
    placed = (
        P("gz", "gy", "gx", None, None),
        P("gz", "gy", "gx", None, None),
        P("gz", "gy", "gx", None, None),
        P("gz", "gy", "gx", None, None),
        P(),
        P(),
    )
    return jax.shard_map(
        functools.partial(shards, sizes),
        mesh=mesh,
        in_specs=placed,
        out_specs=(P("gx", "gy", "gz", None, None), P("gz", "gy", "gx", None, None)),
        check_vma=False,
    )
```
